32 devices in a mesh: seq: 8 (over z, y), tp: 4 (over x, core).
Axes of the slice: x: 2, y: 2, z: 4, core: 2. Of those that a mesh axis runs over, the one named last changes fastest.
Arguments:
- ssm_inputs: bfloat16 [8192, 8192], P('seq', 'tp'), may hold values from -6 to 6
- step_sizes: float32 [8192, 128], P('seq', 'tp'), as said below
- decay_rates: float32 [128], P('tp'), as said below
- state_inputs: bfloat16 [8192, 128], P('seq'), may hold values from -6 to 6
- state_readout: bfloat16 [8192, 128], P('seq'), may hold values from -0.5 to 0.5
- skip_gain: float32 [128], P('tp'), may hold values from 0.5 to 1.5
- mixed_inputs: bfloat16 [1536, 8192], P('seq', 'tp'), may hold values from -6 to 6
- out_weight: bfloat16 [8192, 8192], P('tp', 'seq'), may hold values from -0.0625 to 0.0625
Outputs:
- ssm_output: bfloat16 [8192, 8192], P('seq', 'tp')
- projected: bfloat16 [1536, 8192], P('seq', 'tp')
The draws below stay inside these ranges and needn't reach their ends.
Inputs may be any that keep to these rules, and one draw needn't show every extreme that they name: `step_sizes`: all entries are positive. `decay_rates`: all entries are positive.
All inputs are finite; a program needn't handle non-finite values.
Results may differ from the reference program's by a relative error of at most 0.017.
Values may be sent and summed in bfloat16 or wider, within the bound.
A program may use at most 192 MiB of HBM per device.

```python
import math
import jax
import jax.numpy as jnp
from jax import lax

D = 8192
HEADS = 128
HEAD_DIM = 64
STATE = 128
SPAN = 256
SEQLEN = 8192
TOKENS_B = 1536
INNER = 8192
N_TP = 4


def slow_heads(key):
    share = 0.5
    return jax.random.uniform(jax.random.fold_in(key, 11), (HEADS,)) < share


def draw_step_sizes(key, part):
    slow = slow_heads(key)
    length_root = jnp.sqrt(jnp.float32(SEQLEN))
    base = jnp.where(slow, 2.0 / length_root, 0.15)
    first_key, second_key, third_key = jax.random.split(jax.random.fold_in(key, 21), 3)
    coarse = jnp.exp(jax.random.uniform(first_key, (SEQLEN // 512 + 1, HEADS), minval=math.log(0.5), maxval=math.log(2.0)))
    finer = jnp.exp(jax.random.uniform(second_key, (SEQLEN // 32 + 1, HEADS), minval=math.log(0.6), maxval=math.log(1.6)))
    jitter = jax.random.uniform(third_key, (SEQLEN, HEADS), minval=0.7, maxval=1.4)
    position = jnp.arange(SEQLEN)
    return (base[None, :] * coarse[position // 512] * finer[position // 32] * jitter).astype(jnp.float32)


def draw_decay_rates(key, part):
    slow = slow_heads(key)
    length_root = jnp.sqrt(jnp.float32(SEQLEN))
    first_key, second_key = jax.random.split(jax.random.fold_in(key, 31), 2)
    quick = jnp.exp(jax.random.uniform(first_key, (HEADS,), minval=math.log(0.2), maxval=math.log(0.6)))
    lasting = jnp.exp(jax.random.uniform(second_key, (HEADS,), minval=math.log(0.2), maxval=math.log(0.8))) / (2.0 * length_root)
    return jnp.where(slow, lasting, quick).astype(jnp.float32)


def levels(stream_key, extent, shards, smallest, largest):
    def one(axis_at, blocks):
        draws = jax.random.uniform(jax.random.fold_in(jax.random.fold_in(stream_key, 6), axis_at), (blocks,), jnp.float32, smallest / len(shards), largest / len(shards))
        return jnp.repeat(jnp.exp(draws), extent[axis_at] // blocks).reshape((-1,) + (1,) * (len(extent) - axis_at - 1))

    factor_of = one(*shards[0])
    for cut in shards[1:]:
        factor_of = factor_of * one(*cut)
    return factor_of


def scatter_about(stream_key, dims, spread, bound, cuts=(), kind=jnp.bfloat16):
    array = spread * jax.random.normal(stream_key, dims, jnp.float32)
    if cuts:
        array = array * levels(stream_key, dims, cuts, -0.22, 0.18)
    return jnp.clip(array, -bound, bound).astype(kind)


def setup_inputs(seed: int = 0) -> dict:
    keys = jax.random.split(jax.random.key(seed), 9)
    return {
        "ssm_inputs": scatter_about(keys[0], (SEQLEN, INNER), 1.0, 6.0, ((0, 8), (1, 4))),
        "step_sizes": draw_step_sizes(jax.random.fold_in(keys[8], 71), 0),
        "decay_rates": draw_decay_rates(jax.random.fold_in(keys[8], 71), 0),
        "state_inputs": scatter_about(keys[3], (SEQLEN, STATE), 1.0, 6.0, ((0, 8),)),
        "state_readout": scatter_about(keys[4], (SEQLEN, STATE), STATE ** -0.5, 0.5, ((0, 8),)),
        "skip_gain": jnp.clip(1.0 + 0.1 * jax.random.normal(keys[5], (HEADS,), jnp.float32), 0.5, 1.5),
        "mixed_inputs": scatter_about(keys[6], (TOKENS_B, INNER), 1.0, 6.0, ((0, 8), (1, 4))),
        "out_weight": scatter_about(keys[7], (INNER, D), INNER ** -0.5, 0.0625, ((0, 4), (1, 8))),
    }


def round_keep(value):
    return lax.optimization_barrier(value.astype(jnp.bfloat16)).astype(jnp.float32)


def reference(ssm_inputs, step_sizes, decay_rates, state_inputs, state_readout, skip_gain, mixed_inputs, out_weight):
    block_count = SEQLEN // SPAN
    x_blocks = ssm_inputs.reshape(block_count, SPAN, HEADS, HEAD_DIM)
    dt_blocks = step_sizes.reshape(block_count, SPAN, HEADS)
    b_blocks = state_inputs.reshape(block_count, SPAN, STATE)
    c_blocks = state_readout.reshape(block_count, SPAN, STATE)
    lower = jnp.tril(jnp.ones((SPAN, SPAN), dtype=bool))

    def process_block(carried, block):
        x_block, dt_block, b_block, c_block = block
        x_wide = x_block.astype(jnp.float32)
        log_decay = jnp.cumsum(-decay_rates[None, :] * dt_block, axis=0)
        gram = jnp.dot(c_block, b_block.T, preferred_element_type=jnp.float32)
        per_head = log_decay.T
        differ = per_head[:, :, None] - per_head[:, None, :]
        decay = jnp.exp(jnp.where(lower[None], differ, -jnp.inf))
        scores = round_keep(gram[None] * decay * dt_block.T[:, None, :])
        y_diag = jnp.einsum("hts,shp->thp", scores, x_wide)
        entering = round_keep(carried)
        readout = jnp.einsum("tn,hpn->thp", c_block.astype(jnp.float32), entering)
        y_off = jnp.exp(log_decay)[:, :, None] * readout
        output = (y_diag + y_off + skip_gain[None, :, None] * x_wide).astype(jnp.bfloat16)
        tail_weight = jnp.exp(log_decay[-1][None, :] - log_decay) * dt_block
        weighted = round_keep(tail_weight[:, :, None] * x_wide)
        block_state = jnp.einsum("shp,sn->hpn", weighted, b_block.astype(jnp.float32))
        updated = jnp.exp(log_decay[-1])[:, None, None] * carried + block_state
        return updated, output

    start_state = jnp.zeros((HEADS, HEAD_DIM, STATE), jnp.float32)
    final_state, outputs = lax.scan(process_block, start_state, (x_blocks, dt_blocks, b_blocks, c_blocks))
    ssm_output = outputs.reshape(SEQLEN, HEADS * HEAD_DIM)

    group_width = INNER // N_TP

    def add_group(group, total):
        first = (group * group_width)
        columns = lax.dynamic_slice_in_dim(mixed_inputs, first, group_width, 1)
        rows = lax.dynamic_slice_in_dim(out_weight, first, group_width, 0)
        partial_value = jnp.dot(columns, rows, preferred_element_type=jnp.float32)
        return total + round_keep(partial_value)

    summed = lax.fori_loop(0, N_TP, add_group, jnp.zeros((TOKENS_B, D), jnp.float32))
    projected = summed.astype(jnp.bfloat16)
    return ssm_output, projected
```

```python
import functools

import jax
import jax.numpy as jnp
from jax import lax
from jax.experimental import pallas as pl
from jax.experimental.pallas import tpu as pltpu
from jax.sharding import PartitionSpec as P

HEAD_DIM = 64
STATE = 128
SPAN = 256
PAIR = 2 * HEAD_DIM
GROUP = 8
MESH = pl.DeviceIdType.MESH
F32 = jnp.float32
BF16 = jnp.bfloat16
HIGH = lax.Precision.HIGHEST


def dot(a, b, **kw):
    return jnp.dot(a, b, preferred_element_type=F32, **kw)


def pair_lanes(first, second, rows):
    lane = lax.broadcasted_iota(jnp.int32, (rows, PAIR), 1)
    return jnp.where(
        lane < HEAD_DIM,
        jnp.broadcast_to(first, (rows, PAIR)),
        jnp.broadcast_to(second, (rows, PAIR)),
    )


def states_kernel(
    x_ref, dt_ref, dtt_ref, rate_ref, ratec_ref, bt_ref,
    block_ref, ld_ref, ldt_ref, dec_ref, tot_ref, totdec_ref,
    carry, carry_dec,
):
    block_id = pl.program_id(0)
    heads = dt_ref.shape[1]
    row = lax.broadcasted_iota(jnp.int32, (SPAN, SPAN), 0)
    col = lax.broadcasted_iota(jnp.int32, (SPAN, SPAN), 1)
    lower = (row >= col).astype(F32)
    upper = (row <= col).astype(F32)
    dt = dt_ref[...]
    ld = dot(lower, -rate_ref[...] * dt, precision=HIGH)
    ldt_ref[...] = dot(-ratec_ref[...] * dtt_ref[...], upper, precision=HIGH)
    for g in range(heads // GROUP):
        ld_ref[g] = ld[:, g * GROUP:(g + 1) * GROUP]
    last = ld[SPAN - 1:SPAN, :]
    tail = jnp.exp(last - ld) * dt
    last_dec = jnp.exp(last)

    @pl.when(block_id == 0)
    def _():
        carry[...] = jnp.zeros_like(carry)
        carry_dec[...] = jnp.ones_like(carry_dec)

    bt = bt_ref[...]
    for j in range(heads // 2):
        cols = slice(j * PAIR, (j + 1) * PAIR)
        weight = pair_lanes(tail[:, 2 * j:2 * j + 1], tail[:, 2 * j + 1:2 * j + 2], SPAN)
        weighted = (weight * x_ref[:, cols].astype(F32)).astype(BF16)
        state = dot(bt, weighted)
        block_ref[0, :, cols] = state
        dec = pair_lanes(last_dec[:, 2 * j:2 * j + 1], last_dec[:, 2 * j + 1:2 * j + 2], 8)
        dec_ref[0, :, cols] = dec
        carry[:, cols] = dec[0:1] * carry[:, cols] + state
        carry_dec[:, cols] = dec * carry_dec[:, cols]
    tot_ref[...] = carry[...].astype(BF16)
    totdec_ref[...] = carry_dec[...]


def local_states(x, dt, dtt, rates, bt):
    rows, width = x.shape
    heads = dt.shape[1]
    blocks = rows // SPAN
    groups = heads // GROUP
    return pl.pallas_call(
        states_kernel,
        grid=(blocks,),
        in_specs=[
            pl.BlockSpec((SPAN, width), lambda b: (b, 0)),
            pl.BlockSpec((SPAN, heads), lambda b: (b, 0)),
            pl.BlockSpec((heads, SPAN), lambda b: (0, b)),
            pl.BlockSpec((1, heads), lambda b: (0, 0)),
            pl.BlockSpec((heads, 1), lambda b: (0, 0)),
            pl.BlockSpec((STATE, SPAN), lambda b: (0, b)),
        ],
        out_specs=[
            pl.BlockSpec((1, STATE, width), lambda b: (b, 0, 0)),
            pl.BlockSpec((groups, SPAN, GROUP), lambda b: (0, b, 0)),
            pl.BlockSpec((heads, SPAN), lambda b: (0, b)),
            pl.BlockSpec((1, 8, width), lambda b: (b, 0, 0)),
            pl.BlockSpec((STATE, width), lambda b: (0, 0)),
            pl.BlockSpec((8, width), lambda b: (0, 0)),
        ],
        out_shape=[
            jax.ShapeDtypeStruct((blocks, STATE, width), F32),
            jax.ShapeDtypeStruct((groups, rows, GROUP), F32),
            jax.ShapeDtypeStruct((heads, rows), F32),
            jax.ShapeDtypeStruct((blocks, 8, width), F32),
            jax.ShapeDtypeStruct((STATE, width), BF16),
            jax.ShapeDtypeStruct((8, width), F32),
        ],
        scratch_shapes=[pltpu.VMEM((STATE, width), F32), pltpu.VMEM((8, width), F32)],
        compiler_params=pltpu.CompilerParams(dimension_semantics=("arbitrary",)),
        name="states",
    )(x, dt, dtt, rates[None, :], rates[:, None], bt)


def output_kernel(
    x_ref, dtt_ref, ld_ref, ldt_ref, bt_ref, c_ref, block_ref, dec_ref, before_ref, skip_ref,
    out_ref, carry,
):
    block_id = pl.program_id(0)
    g = pl.program_id(1)
    half = SPAN // 2

    @pl.when(block_id == 0)
    def _():
        carry[g] = before_ref[...]

    entering = carry[g]
    c = c_ref[...]
    readout = dot(c, entering.astype(BF16))
    carry[g] = dec_ref[0, 0:1] * entering + block_ref[0]
    gram = dot(c, bt_ref[...])
    row = lax.broadcasted_iota(jnp.int32, (half, half), 0)
    col = lax.broadcasted_iota(jnp.int32, (half, half), 1)
    lower = row >= col
    gram_top = jnp.where(lower, gram[:half, :half], 0.0)
    gram_low = jnp.where(lower, gram[half:, half:], 0.0)
    gram_off = gram[half:, :half]
    ld = ld_ref[0]
    grow = jnp.exp(ld)
    for j in range(GROUP // 2):
        cols = slice(j * PAIR, (j + 1) * PAIR)
        x = x_ref[:, cols]
        tops, lows = [], []
        for h in (2 * j, 2 * j + 1):
            across = jnp.broadcast_to(ld[:, h:h + 1], (SPAN, half))
            left, right = ldt_ref[h:h + 1, :half], ldt_ref[h:h + 1, half:]
            dt_left, dt_right = dtt_ref[h:h + 1, :half], dtt_ref[h:h + 1, half:]
            top = gram_top * jnp.exp(jnp.minimum(across[:half] - left, 0.0)) * dt_left
            off = gram_off * jnp.exp(jnp.minimum(across[half:] - left, 0.0)) * dt_left
            low = gram_low * jnp.exp(jnp.minimum(across[half:] - right, 0.0)) * dt_right
            tops.append(dot(top.astype(BF16), x[:half]))
            lows.append(
                dot(jnp.concatenate([off.astype(BF16), low.astype(BF16)], axis=1), x)
            )
        lane = lax.broadcasted_iota(jnp.int32, (half, PAIR), 1)
        mine = lane < HEAD_DIM
        scale = pair_lanes(grow[:, 2 * j:2 * j + 1], grow[:, 2 * j + 1:2 * j + 2], SPAN)
        rest = scale * readout[:, cols] + skip_ref[:, cols] * x.astype(F32)
        out_ref[:half, cols] = (jnp.where(mine, tops[0], tops[1]) + rest[:half]).astype(BF16)
        out_ref[half:, cols] = (jnp.where(mine, lows[0], lows[1]) + rest[half:]).astype(BF16)


def scan_output(x, dtt, ld, ldt, bt, c, block_states, dec, before, skip):
    rows, width = x.shape
    blocks = rows // SPAN
    groups = ld.shape[0]
    wide = width // groups
    return pl.pallas_call(
        output_kernel,
        grid=(blocks, groups),
        in_specs=[
            pl.BlockSpec((SPAN, wide), lambda b, g: (b, g)),
            pl.BlockSpec((GROUP, SPAN), lambda b, g: (g, b)),
            pl.BlockSpec((1, SPAN, GROUP), lambda b, g: (g, b, 0)),
            pl.BlockSpec((GROUP, SPAN), lambda b, g: (g, b)),
            pl.BlockSpec((STATE, SPAN), lambda b, g: (0, b)),
            pl.BlockSpec((SPAN, STATE), lambda b, g: (b, 0)),
            pl.BlockSpec((1, STATE, wide), lambda b, g: (b, 0, g)),
            pl.BlockSpec((1, 8, wide), lambda b, g: (b, 0, g)),
            pl.BlockSpec((STATE, wide), lambda b, g: (0, g)),
            pl.BlockSpec((1, wide), lambda b, g: (0, g)),
        ],
        out_specs=pl.BlockSpec((SPAN, wide), lambda b, g: (b, g)),
        out_shape=jax.ShapeDtypeStruct((rows, width), BF16),
        scratch_shapes=[pltpu.VMEM((groups, STATE, wide), F32)],
        compiler_params=pltpu.CompilerParams(dimension_semantics=("arbitrary", "arbitrary")),
        name="scan_output",
    )(x, dtt, ld, ldt, bt, c, block_states, dec, before, skip)


def exchange_kernel(
    n, tps,
    tot_ref, totdec_ref, mixed_ref, weight_ref,
    proj_ref, before_ref,
    cw, ccw, part, red, fin, landed,
    st_out, st_in, dec_out, dec_in, total, total_dec, before_dec,
    ring_send, ring_recv, red_send, red_recv, fin_send, fin_recv, st_send, st_recv,
):
    s = lax.axis_index("seq")
    t = lax.axis_index("tp")
    odd = s % 2
    place = (1 - odd) * (s // 2) + odd * (n - 1 - s // 2)

    def member(at):
        at = (at + 2 * n) % n
        back = at // (n // 2)
        return (1 - back) * (2 * at) + back * (2 * (n - 1 - at) + 1)

    right, left = member(place + 1), member(place - 1)
    rows = mixed_ref.shape[0]
    half = rows // 2
    quarter = rows // tps
    width = weight_ref.shape[1]
    steps = n // 2
    per = n // tps
    rounds = n.bit_length() - 1

    def remote(src, dst, send, recv, where):
        return pltpu.make_async_remote_copy(
            src_ref=src, dst_ref=dst, send_sem=send, recv_sem=recv,
            device_id=where, device_id_type=MESH,
        )

    def hop(way, k, h):
        slots = (cw, ccw)[way]
        span = pl.ds(h * half, half)
        src = mixed_ref.at[span] if k == 0 else slots.at[k - 1, span]
        dst = cw.at[k, span] if k == steps - 1 else slots.at[k, span]
        return remote(
            src, dst, ring_send.at[way, k, h], ring_recv.at[way, k, h],
            {"seq": (right, left)[way]},
        )

    def carries(way, k, h):
        return k < steps and (k < steps - 1 or h == way)

    def passing(r):
        bit = (s // 2 ** r) % 2
        partner = s + (1 - 2 * bit) * 2 ** r
        src = tot_ref if r == 0 else st_out.at[r - 1]
        dec = totdec_ref if r == 0 else dec_out.at[r - 1]
        return bit, (
            remote(src, st_in.at[r], st_send.at[r, 0], st_recv.at[r, 0], {"seq": partner}),
            remote(dec, dec_in.at[r], st_send.at[r, 1], st_recv.at[r, 1], {"seq": partner}),
        )

    def start_round(r):
        bit, copies = passing(r)
        if r < rounds - 1:
            for copy in copies:
                copy.start()
        else:
            @pl.when(bit == 0)
            def _():
                for copy in copies:
                    copy.start()

    def finish_round(r):
        bit, copies = passing(r)

        def lands():
            for copy in copies:
                copy.wait_recv()

        @pl.when(bit == 1)
        def _():
            lands()

            @pl.loop(0, total.shape[1] // 256)
            def _(i):
                cols = pl.ds(pl.multiple_of(i * 256, 256), 256)
                other = st_in[r, :, cols].astype(F32)
                before_ref[:, cols] += before_dec[0:1, cols] * other
                if r < rounds - 1:
                    fresh = total_dec[0:1, cols] * other + total[:, cols]
                    total[:, cols] = fresh
                    st_out[r, :, cols] = fresh.astype(BF16)

            before_dec[...] *= dec_in[r]
            if r < rounds - 1:
                total_dec[...] *= dec_in[r]
                dec_out[r] = total_dec[...]

        if r < rounds - 1:
            @pl.when(bit == 0)
            def _():
                lands()

                @pl.loop(0, total.shape[1] // 256)
                def _(i):
                    cols = pl.ds(pl.multiple_of(i * 256, 256), 256)
                    other = st_in[r, :, cols].astype(F32)
                    fresh = dec_in[r, 0:1, cols] * total[:, cols] + other
                    total[:, cols] = fresh
                    st_out[r, :, cols] = fresh.astype(BF16)

                total_dec[...] *= dec_in[r]
                dec_out[r] = total_dec[...]

            start_round(r + 1)

    def multiply(u, block):
        tile = min(256, width)

        @pl.loop(0, width // tile)
        def _(i):
            cols = pl.ds(pl.multiple_of(i * tile, tile), tile)
            value = dot(block[...], weight_ref[:, cols]).astype(BF16)
            for q in range(tps):
                part[u, q, :, cols] = value[q * quarter:(q + 1) * quarter]

    def reduction(u, j):
        peer = (t + j) % tps
        return remote(
            part.at[u, peer], red.at[u, j - 1], red_send.at[u, j - 1], red_recv.at[u, j - 1],
            {"tp": peer},
        )

    def begin(u, block):
        multiply(u, block)
        for j in range(1, tps):
            reduction(u, j).start()

    def delivery(u, owner):
        return remote(
            fin.at[u], landed.at[s % per, t], fin_send.at[u], fin_recv.at[s % per, t],
            {"seq": owner, "tp": s // per},
        )

    def close(u, owner):
        for j in range(1, tps):
            reduction(u, j).wait_recv()
        value = part[u, t].astype(F32)
        for j in range(1, tps):
            value = value + red[u, j - 1].astype(F32)
        fin[u] = value.astype(BF16)
        if u:
            delivery(u, owner).start()
        else:
            @pl.when(t == s // per)
            def _():
                pltpu.make_async_copy(
                    fin.at[u], landed.at[s % per, t], fin_recv.at[s % per, t]
                ).start()

            @pl.when(t != s // per)
            def _():
                delivery(u, owner).start()

    start_round(0)
    for h in range(2):
        for way in range(2):
            if carries(way, 0, h):
                hop(way, 0, h).start()
    total[...] = tot_ref[...].astype(F32)
    total_dec[...] = totdec_ref[...]
    before_ref[...] = jnp.zeros_like(before_ref)
    before_dec[...] = jnp.ones_like(before_dec)

    begin(0, mixed_ref)
    waiting = [(0, s)]
    done = []
    for k in range(steps):
        if k < rounds:
            finish_round(k)
        for h in range(2):
            for way in range(2):
                if carries(way, k, h):
                    hop(way, k, h).wait_recv()
                    if carries(way, k + 1, h):
                        hop(way, k + 1, h).start()
        fresh = [(1 + 2 * k, member(place - 1 - k))]
        begin(1 + 2 * k, cw.at[k])
        if k < steps - 1:
            begin(2 + 2 * k, ccw.at[k])
            fresh.append((2 + 2 * k, member(place + 1 + k)))
        for u, owner in waiting:
            close(u, owner)
        done += waiting
        waiting = fresh
    for r in range(min(steps, rounds), rounds):
        finish_round(r)
    for u, owner in waiting:
        close(u, owner)
    done += waiting

    for g in range(per):
        for q in range(tps):
            remote(
                fin.at[0], landed.at[g, q], fin_send.at[0], fin_recv.at[g, q], {"seq": right}
            ).wait_recv()
            proj_ref[q * quarter:(q + 1) * quarter, g * width:(g + 1) * width] = landed[g, q]

    for k in range(steps):
        for h in range(2):
            for way in range(2):
                if carries(way, k, h):
                    hop(way, k, h).wait_send()
    for u, owner in done:
        for j in range(1, tps):
            reduction(u, j).wait_send()
        if u:
            delivery(u, owner).wait_send()
        else:
            @pl.when(t != s // per)
            def _():
                delivery(u, owner).wait_send()
    for r in range(rounds):
        bit, copies = passing(r)
        if r < rounds - 1:
            for copy in copies:
                copy.wait_send()
        else:
            @pl.when(bit == 0)
            def _():
                for copy in copies:
                    copy.wait_send()


def exchange(n, tps, tot, totdec, mixed, weight):
    rows, depth = mixed.shape
    width = weight.shape[1]
    quarter = rows // tps
    steps = n // 2
    per = n // tps
    rounds = n.bit_length() - 1
    state = tot.shape
    dec = totdec.shape
    dma = pltpu.SemaphoreType.DMA
    vmem = pl.BlockSpec(memory_space=pltpu.VMEM)
    return pl.pallas_call(
        functools.partial(exchange_kernel, n, tps),
        in_specs=[vmem] * 4,
        out_specs=[vmem] * 2,
        out_shape=[
            jax.ShapeDtypeStruct((rows, per * width), BF16),
            jax.ShapeDtypeStruct(state, F32),
        ],
        scratch_shapes=[
            pltpu.VMEM((steps, rows, depth), BF16),
            pltpu.VMEM((max(steps - 1, 1), rows, depth), BF16),
            pltpu.VMEM((n, tps, quarter, width), BF16),
            pltpu.VMEM((n, tps - 1, quarter, width), BF16),
            pltpu.VMEM((n, quarter, width), BF16),
            pltpu.VMEM((per, tps, quarter, width), BF16),
            pltpu.VMEM((rounds - 1,) + state, BF16),
            pltpu.VMEM((rounds,) + state, BF16),
            pltpu.VMEM((rounds - 1,) + dec, F32),
            pltpu.VMEM((rounds,) + dec, F32),
            pltpu.VMEM(state, F32),
            pltpu.VMEM(dec, F32),
            pltpu.VMEM(dec, F32),
            dma((2, steps, 2)),
            dma((2, steps, 2)),
            dma((n, tps - 1)),
            dma((n, tps - 1)),
            dma((n,)),
            dma((per, tps)),
            dma((rounds, 2)),
            dma((rounds, 2)),
        ],
        compiler_params=pltpu.CompilerParams(
            has_side_effects=True, vmem_limit_bytes=60 * 2 ** 20
        ),
        name="exchange",
    )(tot, totdec, mixed, weight)


def per_device(
    n, tps,
    ssm_inputs,
    step_sizes,
    decay_rates,
    state_inputs,
    state_readout,
    skip_gain,
    mixed_inputs,
    out_weight,
):
    dtt = step_sizes.T
    bt = state_inputs.T
    skip = jnp.repeat(skip_gain, HEAD_DIM)[None, :]
    block_states, ld, ldt, dec, tot, totdec = local_states(
        ssm_inputs, step_sizes, dtt, decay_rates, bt
    )
    projected, before = exchange(n, tps, tot, totdec, mixed_inputs, out_weight)
    ssm_output = scan_output(
        ssm_inputs, dtt, ld, ldt, bt, state_readout, block_states, dec, before, skip
    )
    return (ssm_output, projected)


def solution(mesh):
    in_specs = (
        P("seq", "tp"),
        P("seq", "tp"),
        P("tp"),
        P("seq", None),
        P("seq", None),
        P("tp"),
        P("seq", "tp"),
        P("tp", "seq"),
    )
    out_specs = (P("seq", "tp"), P("seq", "tp"))
    return jax.shard_map(
        functools.partial(per_device, mesh.shape["seq"], mesh.shape["tp"]),
        mesh=mesh, in_specs=in_specs, out_specs=out_specs, check_vma=False,
    )
```

```python
import functools

import jax
import jax.numpy as jnp
from jax import lax
from jax.experimental import pallas as pl
from jax.experimental.pallas import tpu as pltpu
from jax.sharding import PartitionSpec as P

HEAD_DIM = 64
STATE = 128
SPAN = 256
PAIR = 2 * HEAD_DIM
GROUP = 8
MESH = pl.DeviceIdType.MESH
F32 = jnp.float32
BF16 = jnp.bfloat16
HIGH = lax.Precision.HIGHEST


def dot(a, b, **kw):
    return jnp.dot(a, b, preferred_element_type=F32, **kw)


def pair_lanes(first, second, rows):
    lane = lax.broadcasted_iota(jnp.int32, (rows, PAIR), 1)
    return jnp.where(
        lane < HEAD_DIM,
        jnp.broadcast_to(first, (rows, PAIR)),
        jnp.broadcast_to(second, (rows, PAIR)),
    )


def transposed_dot(a, b, **kw):
    return lax.dot_general(a, b, (((0,), (0,)), ((), ())), preferred_element_type=F32, **kw)


def block_prepare(b, x, dt_ref, rate_ref, b_ref, blocks, lds, ldts, dtts, decs, total, total_dec):
    rows = pl.ds(pl.multiple_of(b * SPAN, SPAN), SPAN)
    heads = dt_ref.shape[1]
    row = lax.broadcasted_iota(jnp.int32, (SPAN, SPAN), 0)
    col = lax.broadcasted_iota(jnp.int32, (SPAN, SPAN), 1)
    lower = (row >= col).astype(F32)
    upper = (row <= col).astype(F32)
    same = (row == col).astype(F32)
    dt = dt_ref[rows, :]
    step = -rate_ref[...] * dt
    ld = dot(lower, step, precision=HIGH)
    ldts[b] = transposed_dot(step, upper, precision=HIGH)
    dtts[b] = transposed_dot(dt, same, precision=HIGH)
    for g in range(heads // GROUP):
        lds[b, g] = ld[:, g * GROUP:(g + 1) * GROUP]
    last = ld[SPAN - 1:SPAN, :]
    tail = jnp.exp(last - ld) * dt
    last_dec = jnp.exp(last)
    bt = b_ref[rows, :].astype(F32).T.astype(BF16)
    for j in range(heads // 2):
        cols = slice(j * PAIR, (j + 1) * PAIR)
        weight = pair_lanes(tail[:, 2 * j:2 * j + 1], tail[:, 2 * j + 1:2 * j + 2], SPAN)
        weighted = (weight * x[rows, cols].astype(F32)).astype(BF16)
        state = dot(bt, weighted)
        blocks[b, :, cols] = state
        dec = pair_lanes(last_dec[:, 2 * j:2 * j + 1], last_dec[:, 2 * j + 1:2 * j + 2], 8)
        decs[b, :, cols] = dec
        total[:, cols] = dec[0:1] * total[:, cols] + state
        total_dec[:, cols] = dec * total_dec[:, cols]


def block_inside(b, g, wide, x, b_ref, c_ref, skip_ref, lds, ldts, dtts, diag):
    half = SPAN // 2
    rows = pl.ds(pl.multiple_of(b * SPAN, SPAN), SPAN)
    gram = lax.dot_general(
        c_ref[rows, :], b_ref[rows, :], (((1,), (1,)), ((), ())), preferred_element_type=F32
    )
    row = lax.broadcasted_iota(jnp.int32, (half, half), 0)
    col = lax.broadcasted_iota(jnp.int32, (half, half), 1)
    lower = row >= col
    gram_top = jnp.where(lower, gram[:half, :half], 0.0)
    gram_low = jnp.where(lower, gram[half:, half:], 0.0)
    gram_off = gram[half:, :half]
    ld = lds[b, g]
    heads = pl.ds(pl.multiple_of(g * GROUP, GROUP), GROUP)
    ldt = ldts[b, heads, :]
    dtt = dtts[b, heads, :]
    lane = lax.broadcasted_iota(jnp.int32, (half, PAIR), 1)
    mine = lane < HEAD_DIM
    for j in range(GROUP // 2):
        xs = x[rows, pl.ds(pl.multiple_of(g * wide + j * PAIR, PAIR), PAIR)]
        tops, lows = [], []
        for h in (2 * j, 2 * j + 1):
            across = jnp.broadcast_to(ld[:, h:h + 1], (SPAN, half))
            left, right = ldt[h:h + 1, :half], ldt[h:h + 1, half:]
            dt_left, dt_right = dtt[h:h + 1, :half], dtt[h:h + 1, half:]
            top = gram_top * jnp.exp(jnp.minimum(across[:half] - left, 0.0)) * dt_left
            off = gram_off * jnp.exp(jnp.minimum(across[half:] - left, 0.0)) * dt_left
            low = gram_low * jnp.exp(jnp.minimum(across[half:] - right, 0.0)) * dt_right
            tops.append(dot(top.astype(BF16), xs[:half]))
            lows.append(
                dot(jnp.concatenate([off.astype(BF16), low.astype(BF16)], axis=1), xs)
            )
        skip = skip_ref[:, pl.ds(pl.multiple_of(g * wide + j * PAIR, PAIR), PAIR)]
        rest = skip * xs.astype(F32)
        cols = slice(j * PAIR, (j + 1) * PAIR)
        diag[b, g, :half, cols] = jnp.where(mine, tops[0], tops[1]) + rest[:half]
        diag[b, g, half:, cols] = jnp.where(mine, lows[0], lows[1]) + rest[half:]


def block_finish(b, g, wide, x, c_ref, before, blocks, decs, lds, diag):
    rows = pl.ds(pl.multiple_of(b * SPAN, SPAN), SPAN)
    cols = pl.ds(pl.multiple_of(g * wide, wide), wide)
    entering = before[:, cols]
    readout = dot(c_ref[rows, :], entering.astype(BF16))
    before[:, cols] = decs[b, 0:1, cols] * entering + blocks[b, :, cols]
    grow = jnp.exp(lds[b, g])
    for j in range(GROUP // 2):
        part = slice(j * PAIR, (j + 1) * PAIR)
        scale = pair_lanes(grow[:, 2 * j:2 * j + 1], grow[:, 2 * j + 1:2 * j + 2], SPAN)
        value = diag[b, g, :, part] + scale * readout[:, part]
        x[rows, pl.ds(pl.multiple_of(g * wide + j * PAIR, PAIR), PAIR)] = value.astype(BF16)


def exchange_kernel(
    n, tps,
    x_hbm, dt_ref, rate_ref, b_ref, c_ref, skip_ref, mixed_ref, weight_hbm,
    out_hbm, proj_ref,
    x, weight_ref, blocks, lds, ldts, dtts, decs, diag, before_ref, tot_ref, totdec_ref,
    cw, ccw, part, red, fin, landed,
    st_out, st_in, dec_out, dec_in, total, total_dec, before_dec,
    ring_send, ring_recv, red_send, red_recv, fin_send, fin_recv, st_send, st_recv,
    load, store,
):
    s = lax.axis_index("seq")
    t = lax.axis_index("tp")
    odd = s % 2
    place = (1 - odd) * (s // 2) + odd * (n - 1 - s // 2)

    def member(at):
        at = (at + 2 * n) % n
        back = at // (n // 2)
        return (1 - back) * (2 * at) + back * (2 * (n - 1 - at) + 1)

    right, left = member(place + 1), member(place - 1)
    rows = mixed_ref.shape[0]
    half = rows // 2
    quarter = rows // tps
    width = weight_ref.shape[1]
    steps = n // 2
    per = n // tps
    rounds = n.bit_length() - 1
    block_count, groups = lds.shape[0], lds.shape[1]
    wide = x.shape[1] // groups

    def remote(src, dst, send, recv, where):
        return pltpu.make_async_remote_copy(
            src_ref=src, dst_ref=dst, send_sem=send, recv_sem=recv,
            device_id=where, device_id_type=MESH,
        )

    def hop(way, k, h):
        slots = (cw, ccw)[way]
        span = pl.ds(h * half, half)
        src = mixed_ref.at[span] if k == 0 else slots.at[k - 1, span]
        dst = cw.at[k, span] if k == steps - 1 else slots.at[k, span]
        return remote(
            src, dst, ring_send.at[way, k, h], ring_recv.at[way, k, h],
            {"seq": (right, left)[way]},
        )

    def carries(way, k, h):
        return k < steps and (k < steps - 1 or h == way)

    def combine(r, upper):
        @pl.loop(0, total.shape[1] // 256)
        def _(i):
            cols = pl.ds(pl.multiple_of(i * 256, 256), 256)
            other = st_in[r, :, cols].astype(F32)
            if upper:
                before_ref[:, cols] += before_dec[0:1, cols] * other
            if r < rounds - 1:
                if upper:
                    fresh = total_dec[0:1, cols] * other + total[:, cols]
                else:
                    fresh = dec_in[r, 0:1, cols] * total[:, cols] + other
                total[:, cols] = fresh
                st_out[r, :, cols] = fresh.astype(BF16)

        if upper:
            before_dec[...] *= dec_in[r]
        if r < rounds - 1:
            total_dec[...] *= dec_in[r]
            dec_out[r] = total_dec[...]

    def passing(r):
        bit = (s // 2 ** r) % 2
        partner = s + (1 - 2 * bit) * 2 ** r
        src = tot_ref if r == 0 else st_out.at[r - 1]
        dec = totdec_ref if r == 0 else dec_out.at[r - 1]
        return bit, (
            remote(src, st_in.at[r], st_send.at[r, 0], st_recv.at[r, 0], {"seq": partner}),
            remote(dec, dec_in.at[r], st_send.at[r, 1], st_recv.at[r, 1], {"seq": partner}),
        )

    part_of = s // (n // 4)
    final = rounds - 1

    def onward(own):
        src = st_out.at[final - 1] if own else st_in.at[final]
        dec = dec_out.at[final - 1] if own else dec_in.at[final]
        where = {"seq": (s + n // 4) % n}
        return (
            remote(src, st_in.at[final], st_send.at[final, 0], st_recv.at[final, 0], where),
            remote(dec, dec_in.at[final], st_send.at[final, 1], st_recv.at[final, 1], where),
        )

    def start_round(r):
        if r < final:
            for copy in passing(r)[1]:
                copy.start()
        else:
            @pl.when(part_of == 1)
            def _():
                for copy in onward(True):
                    copy.start()

    def finish_round(r):
        if r < final:
            bit, copies = passing(r)
            for copy in copies:
                copy.wait_recv()

            @pl.when(bit == 1)
            def _():
                combine(r, True)

            @pl.when(bit == 0)
            def _():
                combine(r, False)

            start_round(r + 1)
        else:
            @pl.when(part_of >= 2)
            def _():
                for copy in onward(True):
                    copy.wait_recv()

                @pl.when(part_of == 2)
                def _():
                    for copy in onward(False):
                        copy.start()

                combine(r, True)

    def multiply(u, block):
        tile = min(256, width)

        @pl.loop(0, width // tile)
        def _(i):
            cols = pl.ds(pl.multiple_of(i * tile, tile), tile)
            value = dot(block[...], weight_ref[:, cols]).astype(BF16)
            for q in range(tps):
                part[u, q, :, cols] = value[q * quarter:(q + 1) * quarter]

    def reduction(u, j):
        peer = (t + j) % tps
        return remote(
            part.at[u, peer], red.at[u, j - 1], red_send.at[u, j - 1], red_recv.at[u, j - 1],
            {"tp": peer},
        )

    def begin(u, block):
        multiply(u, block)
        for j in range(1, tps):
            reduction(u, j).start()

    def delivery(u, owner):
        return remote(
            fin.at[u], landed.at[s % per, t], fin_send.at[u], fin_recv.at[s % per, t],
            {"seq": owner, "tp": s // per},
        )

    def close(u, owner):
        for j in range(1, tps):
            reduction(u, j).wait_recv()
        value = part[u, t].astype(F32)
        for j in range(1, tps):
            value = value + red[u, j - 1].astype(F32)
        fin[u] = value.astype(BF16)
        if u:
            delivery(u, owner).start()
        else:
            @pl.when(t == s // per)
            def _():
                pltpu.make_async_copy(
                    fin.at[u], landed.at[s % per, t], fin_recv.at[s % per, t]
                ).start()

            @pl.when(t != s // per)
            def _():
                delivery(u, owner).start()

    x_load = pltpu.make_async_copy(x_hbm, x, load.at[0])
    weight_load = pltpu.make_async_copy(weight_hbm, weight_ref, load.at[1])
    for h in range(2):
        for way in range(2):
            if carries(way, 0, h):
                hop(way, 0, h).start()
    x_load.start()
    weight_load.start()
    total[...] = jnp.zeros_like(total)
    total_dec[...] = jnp.ones_like(total_dec)
    before_ref[...] = jnp.zeros_like(before_ref)
    before_dec[...] = jnp.ones_like(before_dec)
    x_load.wait()

    @pl.loop(0, block_count)
    def _(b):
        block_prepare(
            b, x, dt_ref, rate_ref, b_ref, blocks, lds, ldts, dtts, decs, total, total_dec
        )

    tot_ref[...] = total[...].astype(BF16)
    totdec_ref[...] = total_dec[...]
    start_round(0)
    weight_load.wait()

    def inside(lo, hi):
        if hi > lo:
            @pl.loop(lo, hi)
            def _(u):
                block_inside(
                    u // groups, u % groups, wide, x, b_ref, c_ref, skip_ref,
                    lds, ldts, dtts, diag,
                )

    units = block_count * groups
    slots_left = max(2 * (steps - 1), 1)
    waiting = []
    done = []
    used = 0
    for k in range(steps):
        for h in range(2):
            for way in range(2):
                if carries(way, k, h):
                    hop(way, k, h).wait_recv()
                    if carries(way, k + 1, h):
                        hop(way, k + 1, h).start()
            if k == 0 and h == 0:
                begin(0, mixed_ref)
                waiting = [(0, s)]
            until = min(units, (2 * k + h + 1) * units // slots_left)
            inside(used, until)
            used = until
        fresh = [(1 + 2 * k, member(place - 1 - k))]
        begin(1 + 2 * k, cw.at[k])
        if k < steps - 1:
            begin(2 + 2 * k, ccw.at[k])
            fresh.append((2 + 2 * k, member(place + 1 + k)))
        for u, owner in waiting:
            close(u, owner)
        done += waiting
        waiting = fresh
        if k < rounds and k < steps - 1:
            finish_round(k)
    for r in range(min(steps - 1, rounds), rounds):
        finish_round(r)

    @pl.loop(0, units)
    def _(u):
        block_finish(
            u // groups, u % groups, wide, x, c_ref, before_ref, blocks, decs, lds, diag
        )

    result = pltpu.make_async_copy(x, out_hbm, store.at[0])
    result.start()
    for u, owner in waiting:
        close(u, owner)
    done += waiting

    for g in range(per):
        for q in range(tps):
            remote(
                fin.at[0], landed.at[g, q], fin_send.at[0], fin_recv.at[g, q], {"seq": right}
            ).wait_recv()
            proj_ref[q * quarter:(q + 1) * quarter, g * width:(g + 1) * width] = landed[g, q]

    for k in range(steps):
        for h in range(2):
            for way in range(2):
                if carries(way, k, h):
                    hop(way, k, h).wait_send()
    for u, owner in done:
        for j in range(1, tps):
            reduction(u, j).wait_send()
        if u:
            delivery(u, owner).wait_send()
        else:
            @pl.when(t != s // per)
            def _():
                delivery(u, owner).wait_send()
    for r in range(final):
        for copy in passing(r)[1]:
            copy.wait_send()

    @pl.when(part_of == 1)
    def _():
        for copy in onward(True):
            copy.wait_send()

    @pl.when(part_of == 2)
    def _():
        for copy in onward(False):
            copy.wait_send()

    result.wait()


def layer(n, tps, x, dt, rates, b, c, skip, mixed, weight):
    rows, depth = mixed.shape
    width = weight.shape[1]
    quarter = rows // tps
    steps = n // 2
    per = n // tps
    rounds = n.bit_length() - 1
    length, inner = x.shape
    heads = dt.shape[1]
    blocks = length // SPAN
    groups = heads // GROUP
    state = (STATE, inner)
    dec = (8, inner)
    dma = pltpu.SemaphoreType.DMA
    vmem = pl.BlockSpec(memory_space=pltpu.VMEM)
    hbm = pl.BlockSpec(memory_space=pl.ANY)
    return pl.pallas_call(
        functools.partial(exchange_kernel, n, tps),
        in_specs=[hbm] + [vmem] * 6 + [hbm],
        out_specs=[hbm, vmem],
        out_shape=[
            jax.ShapeDtypeStruct(x.shape, BF16),
            jax.ShapeDtypeStruct((rows, per * width), BF16),
        ],
        scratch_shapes=[
            pltpu.VMEM(x.shape, BF16),
            pltpu.VMEM(weight.shape, BF16),
            pltpu.VMEM((blocks,) + state, F32),
            pltpu.VMEM((blocks, groups, SPAN, GROUP), F32),
            pltpu.VMEM((blocks, heads, SPAN), F32),
            pltpu.VMEM((blocks, heads, SPAN), F32),
            pltpu.VMEM((blocks,) + dec, F32),
            pltpu.VMEM((blocks, groups, SPAN, inner // groups), F32),
            pltpu.VMEM(state, F32),
            pltpu.VMEM(state, BF16),
            pltpu.VMEM(dec, F32),
            pltpu.VMEM((steps, rows, depth), BF16),
            pltpu.VMEM((max(steps - 1, 1), rows, depth), BF16),
            pltpu.VMEM((n, tps, quarter, width), BF16),
            pltpu.VMEM((n, tps - 1, quarter, width), BF16),
            pltpu.VMEM((n, quarter, width), BF16),
            pltpu.VMEM((per, tps, quarter, width), BF16),
            pltpu.VMEM((rounds - 1,) + state, BF16),
            pltpu.VMEM((rounds,) + state, BF16),
            pltpu.VMEM((rounds - 1,) + dec, F32),
            pltpu.VMEM((rounds,) + dec, F32),
            pltpu.VMEM(state, F32),
            pltpu.VMEM(dec, F32),
            pltpu.VMEM(dec, F32),
            dma((2, steps, 2)),
            dma((2, steps, 2)),
            dma((n, tps - 1)),
            dma((n, tps - 1)),
            dma((n,)),
            dma((per, tps)),
            dma((rounds, 2)),
            dma((rounds, 2)),
            dma((2,)),
            dma((1,)),
        ],
        compiler_params=pltpu.CompilerParams(
            has_side_effects=True, vmem_limit_bytes=67_043_328
        ),
        name="layer",
    )(x, dt, rates, b, c, skip, mixed, weight)


def per_device(
    n, tps,
    ssm_inputs,
    step_sizes,
    decay_rates,
    state_inputs,
    state_readout,
    skip_gain,
    mixed_inputs,
    out_weight,
):
    return layer(
        n, tps,
        ssm_inputs, step_sizes, decay_rates[None, :], state_inputs, state_readout,
        jnp.repeat(skip_gain, HEAD_DIM)[None, :], mixed_inputs, out_weight,
    )


def solution(mesh):
    in_specs = (
        P("seq", "tp"),
        P("seq", "tp"),
        P("tp"),
        P("seq", None),
        P("seq", None),
        P("tp"),
        P("seq", "tp"),
        P("tp", "seq"),
    )
    out_specs = (P("seq", "tp"), P("seq", "tp"))
    return jax.shard_map(
        functools.partial(per_device, mesh.shape["seq"], mesh.shape["tp"]),
        mesh=mesh, in_specs=in_specs, out_specs=out_specs, check_vma=False,
    )
```

```python
import functools

import jax
import jax.numpy as jnp
from jax import lax
from jax.experimental import pallas as pl
from jax.experimental.pallas import tpu as pltpu
from jax.sharding import PartitionSpec as P

HEAD_DIM = 64
STATE = 128
SPAN = 256
PAIR = 2 * HEAD_DIM
GROUP = 8
MESH = pl.DeviceIdType.MESH
F32 = jnp.float32
BF16 = jnp.bfloat16
HIGH = lax.Precision.HIGHEST


def dot(a, b, **kw):
    return jnp.dot(a, b, preferred_element_type=F32, **kw)


def pair_lanes(first, second, rows):
    lane = lax.broadcasted_iota(jnp.int32, (rows, PAIR), 1)
    return jnp.where(
        lane < HEAD_DIM,
        jnp.broadcast_to(first, (rows, PAIR)),
        jnp.broadcast_to(second, (rows, PAIR)),
    )


def transposed_dot(a, b, **kw):
    return lax.dot_general(a, b, (((0,), (0,)), ((), ())), preferred_element_type=F32, **kw)


def block_prepare(b, x, dt_ref, rate_ref, b_ref, blocks, lds, ldts, dtts, decs, total, total_dec):
    rows = pl.ds(pl.multiple_of(b * SPAN, SPAN), SPAN)
    heads = dt_ref.shape[1]
    row = lax.broadcasted_iota(jnp.int32, (SPAN, SPAN), 0)
    col = lax.broadcasted_iota(jnp.int32, (SPAN, SPAN), 1)
    lower = (row >= col).astype(F32)
    upper = (row <= col).astype(F32)
    same = (row == col).astype(F32)
    dt = dt_ref[rows, :]
    step = -rate_ref[...] * dt
    ld = dot(lower, step, precision=HIGH)
    ldts[b] = transposed_dot(step, upper, precision=HIGH)
    dtts[b] = transposed_dot(dt, same, precision=HIGH)
    for g in range(heads // GROUP):
        lds[b, g] = ld[:, g * GROUP:(g + 1) * GROUP]
    last = ld[SPAN - 1:SPAN, :]
    tail = jnp.exp(last - ld) * dt
    last_dec = jnp.exp(last)
    bt = b_ref[rows, :].astype(F32).T.astype(BF16)
    for j in range(heads // 2):
        cols = slice(j * PAIR, (j + 1) * PAIR)
        weight = pair_lanes(tail[:, 2 * j:2 * j + 1], tail[:, 2 * j + 1:2 * j + 2], SPAN)
        weighted = (weight * x[rows, cols].astype(F32)).astype(BF16)
        state = dot(bt, weighted)
        blocks[b, :, cols] = state
        dec = pair_lanes(last_dec[:, 2 * j:2 * j + 1], last_dec[:, 2 * j + 1:2 * j + 2], 8)
        decs[b, :, cols] = dec
        total[:, cols] = dec[0:1] * total[:, cols] + state
        total_dec[:, cols] = dec * total_dec[:, cols]


def block_inside(b, g, wide, x, b_ref, c_ref, skip_ref, lds, ldts, dtts, diag):
    half = SPAN // 2
    rows = pl.ds(pl.multiple_of(b * SPAN, SPAN), SPAN)
    gram = lax.dot_general(
        c_ref[rows, :], b_ref[rows, :], (((1,), (1,)), ((), ())), preferred_element_type=F32
    )
    row = lax.broadcasted_iota(jnp.int32, (half, half), 0)
    col = lax.broadcasted_iota(jnp.int32, (half, half), 1)
    lower = row >= col
    gram_top = jnp.where(lower, gram[:half, :half], 0.0)
    gram_low = jnp.where(lower, gram[half:, half:], 0.0)
    gram_off = gram[half:, :half]
    ld = lds[b, g]
    heads = pl.ds(pl.multiple_of(g * GROUP, GROUP), GROUP)
    ldt = ldts[b, heads, :]
    dtt = dtts[b, heads, :]
    lane = lax.broadcasted_iota(jnp.int32, (half, PAIR), 1)
    mine = lane < HEAD_DIM
    for j in range(GROUP // 2):
        xs = x[rows, pl.ds(pl.multiple_of(g * wide + j * PAIR, PAIR), PAIR)]
        tops, lows = [], []
        for h in (2 * j, 2 * j + 1):
            across = jnp.broadcast_to(ld[:, h:h + 1], (SPAN, half))
            left, right = ldt[h:h + 1, :half], ldt[h:h + 1, half:]
            dt_left, dt_right = dtt[h:h + 1, :half], dtt[h:h + 1, half:]
            top = gram_top * jnp.exp(jnp.minimum(across[:half] - left, 0.0)) * dt_left
            off = gram_off * jnp.exp(jnp.minimum(across[half:] - left, 0.0)) * dt_left
            low = gram_low * jnp.exp(jnp.minimum(across[half:] - right, 0.0)) * dt_right
            tops.append(dot(top.astype(BF16), xs[:half]))
            lows.append(
                dot(jnp.concatenate([off.astype(BF16), low.astype(BF16)], axis=1), xs)
            )
        skip = skip_ref[:, pl.ds(pl.multiple_of(g * wide + j * PAIR, PAIR), PAIR)]
        rest = skip * xs.astype(F32)
        cols = slice(j * PAIR, (j + 1) * PAIR)
        diag[b, g, :half, cols] = jnp.where(mine, tops[0], tops[1]) + rest[:half]
        diag[b, g, half:, cols] = jnp.where(mine, lows[0], lows[1]) + rest[half:]


def block_finish(b, g, wide, x, c_ref, before, blocks, decs, lds, diag):
    rows = pl.ds(pl.multiple_of(b * SPAN, SPAN), SPAN)
    cols = pl.ds(pl.multiple_of(g * wide, wide), wide)
    entering = before[:, cols]
    readout = dot(c_ref[rows, :], entering.astype(BF16))
    before[:, cols] = decs[b, 0:1, cols] * entering + blocks[b, :, cols]
    grow = jnp.exp(lds[b, g])
    for j in range(GROUP // 2):
        part = slice(j * PAIR, (j + 1) * PAIR)
        scale = pair_lanes(grow[:, 2 * j:2 * j + 1], grow[:, 2 * j + 1:2 * j + 2], SPAN)
        value = diag[b, g, :, part] + scale * readout[:, part]
        x[rows, pl.ds(pl.multiple_of(g * wide + j * PAIR, PAIR), PAIR)] = value.astype(BF16)


def exchange_kernel(
    n, tps,
    x_hbm, dt_ref, rate_ref, b_ref, c_ref, skip_ref, mixed_ref, weight_hbm,
    out_hbm, proj_ref,
    x, weight_ref, blocks, lds, ldts, dtts, decs, diag, before_ref, tot_ref, totdec_ref,
    cw, ccw, part, red, fin, landed,
    st_out, st_in, dec_in, total, total_dec, before_dec,
    ring_send, ring_recv, red_send, red_recv, fin_send, fin_recv, st_send, st_recv,
    load, store,
):
    s = lax.axis_index("seq")
    t = lax.axis_index("tp")
    odd = s % 2
    place = (1 - odd) * (s // 2) + odd * (n - 1 - s // 2)

    def member(at):
        at = (at + 2 * n) % n
        back = at // (n // 2)
        return (1 - back) * (2 * at) + back * (2 * (n - 1 - at) + 1)

    right, left = member(place + 1), member(place - 1)
    rows = mixed_ref.shape[0]
    half = rows // 2
    quarter = rows // tps
    width = weight_ref.shape[1]
    steps = n // 2
    per = n // tps
    block_count, groups = lds.shape[0], lds.shape[1]
    wide = x.shape[1] // groups

    def remote(src, dst, send, recv, where):
        return pltpu.make_async_remote_copy(
            src_ref=src, dst_ref=dst, send_sem=send, recv_sem=recv,
            device_id=where, device_id_type=MESH,
        )

    def hop(way, k, h):
        slots = (cw, ccw)[way]
        span = pl.ds(h * half, half)
        src = mixed_ref.at[span] if k == 0 else slots.at[k - 1, span]
        dst = cw.at[k, span] if k == steps - 1 else slots.at[k, span]
        return remote(
            src, dst, ring_send.at[way, k, h], ring_recv.at[way, k, h],
            {"seq": (right, left)[way]},
        )

    def carries(way, k, h):
        return k < steps and (k < steps - 1 or h == way)

    pair, side = s // 2, s % 2
    pairs = n // 2
    share = total.shape[1] // 2

    def swap():
        where = {"seq": s + 1 - 2 * side}
        return (
            remote(tot_ref, st_in.at[0], st_send.at[0], st_recv.at[0], where),
            remote(totdec_ref, dec_in, st_send.at[1], st_recv.at[1], where),
        )

    def chain():
        cols = pl.ds(pl.multiple_of(side * share, share), share)
        return remote(
            st_out.at[:, cols], st_in.at[1, :, cols], st_send.at[2], st_recv.at[2],
            {"seq": (s + 2) % n},
        )

    def mirror():
        cols = pl.ds(pl.multiple_of(side * share, share), share)
        part_ref = st_in.at[1, :, cols]
        return remote(
            part_ref, part_ref, st_send.at[3], st_recv.at[3], {"seq": s + 1 - 2 * side}
        )

    def mirrored():
        cols = pl.ds(pl.multiple_of((1 - side) * share, share), share)
        part_ref = st_in.at[1, :, cols]
        return remote(
            part_ref, part_ref, st_send.at[3], st_recv.at[3], {"seq": s + 1 - 2 * side}
        )

    def join_pair():
        for copy in swap():
            copy.wait_recv()
        mine = side.astype(F32)

        @pl.loop(0, total.shape[1] // 256)
        def _(i):
            cols = pl.ds(pl.multiple_of(i * 256, 256), 256)
            other = st_in[0, :, cols].astype(F32)
            own = total[:, cols]
            before_ref[:, cols] = mine * other
            upper = total_dec[0:1, cols] * other + own
            under = dec_in[0:1, cols] * own + other
            fresh = mine * upper + (1.0 - mine) * under
            total[:, cols] = fresh

        before_dec[...] = mine * dec_in[...] + (1.0 - mine)
        total_dec[...] = total_dec[...] * dec_in[...]

        @pl.when(pair == 0)
        def _():
            st_out[...] = total[...].astype(BF16)
            chain().start()

    def link(q):
        @pl.when(pair == q)
        def _():
            chain().wait_recv()
            if q < pairs - 1:
                cols = pl.ds(pl.multiple_of(side * share, share), share)
                st_out[:, cols] = (
                    total_dec[0:1, cols] * st_in[1, :, cols].astype(F32) + total[:, cols]
                ).astype(BF16)
                chain().start()
            mirror().start()

    def join_all():
        @pl.when(pair > 0)
        def _():
            mirrored().wait_recv()

            @pl.loop(0, total.shape[1] // 256)
            def _(i):
                cols = pl.ds(pl.multiple_of(i * 256, 256), 256)
                before_ref[:, cols] += before_dec[0:1, cols] * st_in[1, :, cols].astype(F32)

    def multiply(u, block):
        tile = min(256, width)

        @pl.loop(0, width // tile)
        def _(i):
            cols = pl.ds(pl.multiple_of(i * tile, tile), tile)
            value = dot(block[...], weight_ref[:, cols]).astype(BF16)
            for q in range(tps):
                part[u, q, :, cols] = value[q * quarter:(q + 1) * quarter]

    def reduction(u, j):
        peer = (t + j) % tps
        return remote(
            part.at[u, peer], red.at[u, j - 1], red_send.at[u, j - 1], red_recv.at[u, j - 1],
            {"tp": peer},
        )

    def begin(u, block):
        multiply(u, block)
        for j in range(1, tps):
            reduction(u, j).start()

    def delivery(u, owner):
        return remote(
            fin.at[u], landed.at[s % per, t], fin_send.at[u], fin_recv.at[s % per, t],
            {"seq": owner, "tp": s // per},
        )

    def close(u, owner):
        for j in range(1, tps):
            reduction(u, j).wait_recv()
        value = part[u, t].astype(F32)
        for j in range(1, tps):
            value = value + red[u, j - 1].astype(F32)
        fin[u] = value.astype(BF16)
        if u:
            delivery(u, owner).start()
        else:
            @pl.when(t == s // per)
            def _():
                pltpu.make_async_copy(
                    fin.at[u], landed.at[s % per, t], fin_recv.at[s % per, t]
                ).start()

            @pl.when(t != s // per)
            def _():
                delivery(u, owner).start()

    x_load = pltpu.make_async_copy(x_hbm, x, load.at[0])
    weight_load = pltpu.make_async_copy(weight_hbm, weight_ref, load.at[1])
    for h in range(2):
        for way in range(2):
            if carries(way, 0, h):
                hop(way, 0, h).start()
    x_load.start()
    weight_load.start()
    total[...] = jnp.zeros_like(total)
    total_dec[...] = jnp.ones_like(total_dec)
    before_ref[...] = jnp.zeros_like(before_ref)
    before_dec[...] = jnp.ones_like(before_dec)
    x_load.wait()

    @pl.loop(0, block_count)
    def _(b):
        block_prepare(
            b, x, dt_ref, rate_ref, b_ref, blocks, lds, ldts, dtts, decs, total, total_dec
        )

    tot_ref[...] = total[...].astype(BF16)
    totdec_ref[...] = total_dec[...]
    for copy in swap():
        copy.start()
    weight_load.wait()

    def inside(lo, hi):
        if hi > lo:
            @pl.loop(lo, hi)
            def _(u):
                block_inside(
                    u // groups, u % groups, wide, x, b_ref, c_ref, skip_ref,
                    lds, ldts, dtts, diag,
                )

    units = block_count * groups
    slots_left = max(2 * (steps - 1), 1)
    waiting = []
    done = []
    used = 0
    for k in range(steps):
        for h in range(2):
            for way in range(2):
                if carries(way, k, h):
                    hop(way, k, h).wait_recv()
                    if carries(way, k + 1, h):
                        hop(way, k + 1, h).start()
            if k == 0 and h == 0:
                begin(0, mixed_ref)
                waiting = [(0, s)]
            if 2 * k + h == 1:
                join_pair()
            if 1 <= 2 * k + h - 2 < pairs:
                link(2 * k + h - 2)
            until = min(units, (2 * k + h + 1) * units // slots_left)
            inside(used, until)
            used = until
        fresh = [(1 + 2 * k, member(place - 1 - k))]
        begin(1 + 2 * k, cw.at[k])
        if k < steps - 1:
            begin(2 + 2 * k, ccw.at[k])
            fresh.append((2 + 2 * k, member(place + 1 + k)))
        for u, owner in waiting:
            close(u, owner)
        done += waiting
        waiting = fresh
    for u, owner in waiting:
        close(u, owner)
    done += waiting
    join_all()

    @pl.loop(0, units)
    def _(u):
        block_finish(
            u // groups, u % groups, wide, x, c_ref, before_ref, blocks, decs, lds, diag
        )

    result = pltpu.make_async_copy(x, out_hbm, store.at[0])
    result.start()

    for g in range(per):
        for q in range(tps):
            remote(
                fin.at[0], landed.at[g, q], fin_send.at[0], fin_recv.at[g, q], {"seq": right}
            ).wait_recv()
            proj_ref[q * quarter:(q + 1) * quarter, g * width:(g + 1) * width] = landed[g, q]

    for k in range(steps):
        for h in range(2):
            for way in range(2):
                if carries(way, k, h):
                    hop(way, k, h).wait_send()
    for u, owner in done:
        for j in range(1, tps):
            reduction(u, j).wait_send()
        if u:
            delivery(u, owner).wait_send()
        else:
            @pl.when(t != s // per)
            def _():
                delivery(u, owner).wait_send()
    for copy in swap():
        copy.wait_send()

    @pl.when(pair < pairs - 1)
    def _():
        chain().wait_send()

    @pl.when(pair > 0)
    def _():
        mirror().wait_send()

    result.wait()


def layer(n, tps, x, dt, rates, b, c, skip, mixed, weight):
    rows, depth = mixed.shape
    width = weight.shape[1]
    quarter = rows // tps
    steps = n // 2
    per = n // tps
    length, inner = x.shape
    heads = dt.shape[1]
    blocks = length // SPAN
    groups = heads // GROUP
    state = (STATE, inner)
    dec = (8, inner)
    dma = pltpu.SemaphoreType.DMA
    vmem = pl.BlockSpec(memory_space=pltpu.VMEM)
    hbm = pl.BlockSpec(memory_space=pl.ANY)
    return pl.pallas_call(
        functools.partial(exchange_kernel, n, tps),
        in_specs=[hbm] + [vmem] * 6 + [hbm],
        out_specs=[hbm, vmem],
        out_shape=[
            jax.ShapeDtypeStruct(x.shape, BF16),
            jax.ShapeDtypeStruct((rows, per * width), BF16),
        ],
        scratch_shapes=[
            pltpu.VMEM(x.shape, BF16),
            pltpu.VMEM(weight.shape, BF16),
            pltpu.VMEM((blocks,) + state, F32),
            pltpu.VMEM((blocks, groups, SPAN, GROUP), F32),
            pltpu.VMEM((blocks, heads, SPAN), F32),
            pltpu.VMEM((blocks, heads, SPAN), F32),
            pltpu.VMEM((blocks,) + dec, F32),
            pltpu.VMEM((blocks, groups, SPAN, inner // groups), F32),
            pltpu.VMEM(state, F32),
            pltpu.VMEM(state, BF16),
            pltpu.VMEM(dec, F32),
            pltpu.VMEM((steps, rows, depth), BF16),
            pltpu.VMEM((max(steps - 1, 1), rows, depth), BF16),
            pltpu.VMEM((n, tps, quarter, width), BF16),
            pltpu.VMEM((n, tps - 1, quarter, width), BF16),
            pltpu.VMEM((n, quarter, width), BF16),
            pltpu.VMEM((per, tps, quarter, width), BF16),
            pltpu.VMEM(state, BF16),
            pltpu.VMEM((2,) + state, BF16),
            pltpu.VMEM(dec, F32),
            pltpu.VMEM(state, F32),
            pltpu.VMEM(dec, F32),
            pltpu.VMEM(dec, F32),
            dma((2, steps, 2)),
            dma((2, steps, 2)),
            dma((n, tps - 1)),
            dma((n, tps - 1)),
            dma((n,)),
            dma((per, tps)),
            dma((4,)),
            dma((4,)),
            dma((2,)),
            dma((1,)),
        ],
        compiler_params=pltpu.CompilerParams(
            has_side_effects=True, vmem_limit_bytes=67_043_328
        ),
        name="layer",
    )(x, dt, rates, b, c, skip, mixed, weight)


def per_device(
    n, tps,
    ssm_inputs,
    step_sizes,
    decay_rates,
    state_inputs,
    state_readout,
    skip_gain,
    mixed_inputs,
    out_weight,
):
    return layer(
        n, tps,
        ssm_inputs, step_sizes, decay_rates[None, :], state_inputs, state_readout,
        jnp.repeat(skip_gain, HEAD_DIM)[None, :], mixed_inputs, out_weight,
    )


def solution(mesh):
    in_specs = (
        P("seq", "tp"),
        P("seq", "tp"),
        P("tp"),
        P("seq", None),
        P("seq", None),
        P("tp"),
        P("seq", "tp"),
        P("tp", "seq"),
    )
    out_specs = (P("seq", "tp"), P("seq", "tp"))
    return jax.shard_map(
        functools.partial(per_device, mesh.shape["seq"], mesh.shape["tp"]),
        mesh=mesh, in_specs=in_specs, out_specs=out_specs, check_vma=False,
    )
```
